32 devices in a mesh: ep: 8 (over z, y), tp: 4 (over x, core).
Axes of the slice: x: 2, y: 2, z: 4, core: 2. Of those that a mesh axis runs over, the one named last changes fastest.
Arguments:
- tokens: bfloat16 [4096, 2048], P(('ep', 'tp')), may hold values from -6 to 6
- norm_gain: float32 [2048], replicated, may hold values from 0.1 to 1.9
- expert_ids: int32 [4096, 6], P(('ep', 'tp')), may hold values from 0 to 15, as said below
- slot_index: int32 [4096, 6], P(('ep', 'tp')), may hold values from 0 to 63, as said below
- dropped: int32 [4096, 6], P(('ep', 'tp')), may hold values from 0 to 1, as said below
- gates: float32 [4096, 6], P(('ep', 'tp')), may hold values from 0.05 to 0.8
- w_gate: bfloat16 [16, 2048, 704], P('ep', None, 'tp'), may hold values from -0.125 to 0.125
- w_up: bfloat16 [16, 2048, 704], P('ep', None, 'tp'), may hold values from -0.125 to 0.125
- w_down: bfloat16 [16, 2048, 704], P('ep', None, 'tp'), may hold values from -0.21875 to 0.21875
- shared_gate: bfloat16 [2048, 1408], P(None, 'tp'), may hold values from -0.125 to 0.125
- shared_up: bfloat16 [2048, 1408], P(None, 'tp'), may hold values from -0.125 to 0.125
- shared_down: bfloat16 [1408, 2048], replicated, may hold values from -0.15625 to 0.15625
Outputs:
- layer_out: bfloat16 [4096, 2048], P(('ep', 'tp'))
The draws below stay inside these ranges and needn't reach their ends.
Inputs may be any that keep to these rules, and one draw needn't show every extreme that they name: `expert_ids`: each token names 6 different experts; some expert has 64 kept pairs from the tokens of every device. `slot_index`: for a kept pair, its place among the slots of its expert for the tokens of its device (the tokens n with one value of n // 128); the kept pairs of one device and one expert have distinct places; 0 for a dropped pair. `dropped`: 1 for the pairs of a device and an expert beyond the 64 that are kept.
All inputs are finite; a program needn't handle non-finite values.
Results may differ from the reference program's by a relative error of at most 0.0054.
Values may be sent and summed in bfloat16 or wider, within the bound.
A program may use at most 128 MiB of HBM per device.

```python
import math
import jax
import jax.numpy as jnp
from jax import lax

D = 2048
FF = 704
SFF = 1408
TOP = 6
TOK_DEV = 128
SPECIALIST_NETS = 16
SEQUENCE_ITEMS = 4096
CAP = 64


def routing_tables(key):
    base = jax.random.fold_in(key, 4242)
    key_noise, key_hot, key_first, key_offset = jax.random.split(base, 4)
    blocks = SEQUENCE_ITEMS // TOK_DEV
    random_perturbation = jax.random.randint(key_noise, (SEQUENCE_ITEMS, SPECIALIST_NETS), 0, 65536, dtype=jnp.int32)
    hot_count = max(1, SPECIALIST_NETS // 16)
    favoured_specialists = jax.random.permutation(key_hot, SPECIALIST_NETS)[:hot_count]
    favoured_increment = jnp.zeros((SPECIALIST_NETS,), jnp.int32).at[favoured_specialists].set(16384)
    first_expert = jax.random.randint(key_first, (), 0, SPECIALIST_NETS, dtype=jnp.int32)
    offsets = jax.random.randint(key_offset, (blocks,), 0, TOK_DEV, dtype=jnp.int32)
    positions = jnp.arange(SEQUENCE_ITEMS, dtype=jnp.int32)
    within = jnp.mod(positions % TOK_DEV - offsets[positions // TOK_DEV], TOK_DEV)
    forced = within < 2 * CAP
    matrix_breadth = jnp.arange(SPECIALIST_NETS, dtype=jnp.int32)
    gating_scores = (random_perturbation + favoured_increment[None, :]) * SPECIALIST_NETS + matrix_breadth[None, :]
    gating_scores = gating_scores + jnp.where(forced[:, None] & (matrix_breadth[None, :] == first_expert), 1 << 30, 0).astype(jnp.int32)
    chosen = lax.top_k(gating_scores, TOP)[1].astype(jnp.int32)
    pairs = chosen.reshape(blocks, TOK_DEV * TOP)
    onehot = (pairs[:, :, None] == matrix_breadth[None, None, :]).astype(jnp.int32)
    rank_table = jnp.sum(jnp.cumsum(onehot, axis=1) * onehot, axis=2) - 1
    rank_table = rank_table.reshape(SEQUENCE_ITEMS, TOP)
    dropped_pairs = (rank_table >= CAP).astype(jnp.int32)
    slots = jnp.where(rank_table >= CAP, 0, rank_table).astype(jnp.int32)
    return (chosen, slots, dropped_pairs)


def draw_expert_ids(key, part):
    return routing_tables(key)[0]


def draw_slot_index(key, part):
    return routing_tables(key)[1]


def draw_dropped(key, part):
    return routing_tables(key)[2]


def block_scale(own_key, dims, shards, least, top_value):
    factor_of = 1.0
    for axis_at, shards_of in shards:
        steps = jax.random.uniform(jax.random.fold_in(jax.random.fold_in(own_key, 6), axis_at), (shards_of,), jnp.float32, least / len(shards), top_value / len(shards))
        factor_of = factor_of * jnp.repeat(jnp.exp(steps), dims[axis_at] // shards_of).reshape((-1,) + (1,) * (len(dims) - 1 - axis_at))
    return factor_of


def gaussian(stream_key, dims, spread, bound, cuts=(), kind=jnp.bfloat16):
    values = jax.random.normal(stream_key, dims, jnp.float32) * spread
    if len(cuts) > 0:
        values = block_scale(stream_key, dims, cuts, -0.22, 0.18) * values
    return jnp.clip(values, min=-bound, max=bound).astype(kind)


def setup_inputs(seed: int = 0) -> dict:
    streams_of = jax.random.split(jax.random.key(seed), 13)
    return {
        "tokens": gaussian(streams_of[0], (SEQUENCE_ITEMS, D), 1.0, 6.0, ((0, 32),)),
        "norm_gain": jnp.clip(1.0 + 0.18 * jax.random.normal(streams_of[1], (D,), jnp.float32), 0.1, 1.9),
        "expert_ids": draw_expert_ids(jax.random.fold_in(streams_of[12], 71), 0),
        "slot_index": draw_slot_index(jax.random.fold_in(streams_of[12], 71), 0),
        "dropped": draw_dropped(jax.random.fold_in(streams_of[12], 71), 0),
        "gates": jnp.clip(jnp.exp(math.log(0.8) - 2.7725887 * jax.random.uniform(streams_of[5], (SEQUENCE_ITEMS, TOP), jnp.float32) ** block_scale(streams_of[5], (SEQUENCE_ITEMS, TOP), ((0, 32),), -0.2, 0.2)), 0.05, 0.8),
        "w_gate": gaussian(streams_of[6], (SPECIALIST_NETS, D, FF), D ** -0.5, 0.125, ((0, 8), (2, 4))),
        "w_up": gaussian(streams_of[7], (SPECIALIST_NETS, D, FF), D ** -0.5, 0.125, ((0, 8), (2, 4))),
        "w_down": gaussian(streams_of[8], (SPECIALIST_NETS, D, FF), FF ** -0.5, 0.21875, ((0, 8), (2, 4))),
        "shared_gate": gaussian(streams_of[9], (D, SFF), D ** -0.5, 0.125, ((1, 4),)),
        "shared_up": gaussian(streams_of[10], (D, SFF), D ** -0.5, 0.125, ((1, 4),)),
        "shared_down": gaussian(streams_of[11], (SFF, D), SFF ** -0.5, 0.15625),
    }


norm_eps = 1e-06

def swiglu(left, right):
    return jax.nn.silu(left) * right

def reference(tokens, norm_gain, expert_ids, slot_index, dropped, gates, w_gate, w_up, w_down, shared_gate, shared_up, shared_down):
    values = tokens.astype(jnp.float32)
    scale = lax.rsqrt(lax.optimization_barrier(jnp.mean(values * values, axis=-1, keepdims=True)) + norm_eps)
    normed = (values * scale * norm_gain).astype(jnp.bfloat16)
    shared_gate_act = jnp.dot(normed, shared_gate, preferred_element_type=jnp.float32)
    shared_up_act = jnp.dot(normed, shared_up, preferred_element_type=jnp.float32)
    shared_hidden = swiglu(shared_gate_act, shared_up_act).astype(jnp.bfloat16)
    shared_out = jnp.dot(shared_hidden, shared_down, preferred_element_type=jnp.float32)
    blocks = SEQUENCE_ITEMS // TOK_DEV
    width = blocks * CAP
    token_index = jnp.broadcast_to(jnp.arange(SEQUENCE_ITEMS, dtype=jnp.int32)[:, None], (SEQUENCE_ITEMS, TOP))
    slot_row = expert_ids * width + token_index // TOK_DEV * CAP + slot_index
    slot_row = jnp.where(dropped == 0, slot_row, SPECIALIST_NETS * width).astype(jnp.int32)
    owner = jnp.full((SPECIALIST_NETS * width + 1,), SEQUENCE_ITEMS, jnp.int32)
    owner = owner.at[slot_row.reshape(-1)].set(token_index.reshape(-1).astype(jnp.int32))
    kept_gates = jnp.where(dropped == 0, gates, jnp.float32(0.0)).astype(jnp.float32)
    weight_table = jnp.zeros((SPECIALIST_NETS * width + 1,), jnp.float32).at[slot_row.reshape(-1)].set(kept_gates.reshape(-1))
    owner = owner[:-1].reshape(SPECIALIST_NETS, width)
    weight_table = weight_table[:-1].reshape(SPECIALIST_NETS, width)
    padded = jnp.concatenate([normed, jnp.zeros((1, D), jnp.bfloat16)], axis=0)

    def one_expert(running, inputs):
        picked, weights, gate_mat, up_mat, down_mat = inputs
        picked_rows = padded[picked].astype(jnp.float32)
        gate_act = jnp.dot(picked_rows, gate_mat.astype(jnp.float32), precision=lax.Precision.HIGHEST)
        up_act = jnp.dot(picked_rows, up_mat.astype(jnp.float32), precision=lax.Precision.HIGHEST)
        hidden = lax.optimization_barrier(swiglu(gate_act, up_act).astype(jnp.bfloat16)).astype(jnp.float32)
        expert_out = jnp.dot(hidden, down_mat.astype(jnp.float32).T, precision=lax.Precision.HIGHEST)
        expert_out = lax.optimization_barrier(expert_out.astype(jnp.bfloat16)).astype(jnp.float32)
        running = running.at[picked].add(weights[:, None] * expert_out)
        return (running, None)
    start = jnp.zeros((SEQUENCE_ITEMS + 1, D), jnp.float32)
    running, _ = lax.scan(one_expert, start, (owner, weight_table, w_gate, w_up, w_down))
    routed = running[:SEQUENCE_ITEMS]
    return (values + shared_out + routed).astype(jnp.bfloat16)
```

```python
import functools

import jax
import jax.numpy as jnp
from jax import lax
from jax.experimental import pallas as pl
from jax.experimental.pallas import tpu as pltpu
from jax.sharding import PartitionSpec as P

MESH = pl.DeviceIdType.MESH
CORES = 2
COLS = 2
VMEM_BYTES = 62 * 1024 * 1024
LANES = 128

NT = (((1,), (1,)), ((), ()))
NN = (((1,), (0,)), ((), ()))


def dot(a, b, dims):
    return lax.dot_general(a, b, dims, preferred_element_type=jnp.float32)


def flip(index, mask, size):
    out, bit = 0, 1
    while bit < size:
        digit = (index // bit) % 2
        out = out + (1 - digit if mask & bit else digit) * bit
        bit *= 2
    return out


def cuts_of(width):
    inside = width - 4 * LANES
    sizes = [LANES] * 2 + [2 * LANES] * (inside // (2 * LANES)) + [LANES] * 2
    starts = [sum(sizes[:i]) for i in range(len(sizes))]
    return [pl.ds(*cut) for cut in zip(starts, sizes)]


def layer_kernel(
    n_rows_z,
    tokens_in,
    gain_in,
    ids_in,
    dropped_in,
    gates_in,
    w_gate,
    w_up,
    w_down,
    s_gate,
    s_up,
    s_down,
    result,
    tokens,
    gain,
    ids,
    dropped,
    gates,
    out,
    xb,
    wtb,
    gu,
    ga0,
    ga1,
    db,
    hb,
    hl0,
    hl1,
    sb,
    sg,
    su,
    sd,
    sh,
    whid,
    ysend,
    yrecv,
    ypart,
    zsend,
    zrecv,
    own_sem,
    near_send,
    near_recv,
    far_send,
    far_recv,
    pass_send,
    pass_recv,
    z_send,
    z_recv,
    y_send,
    y_recv,
    t_send,
    t_recv,
    h_send,
    h_recv,
    ry_send,
    ry_recv,
    rz_send,
    rz_join,
    rz_recv,
    go,
    in_sem,
    out_sem,
):
    ep, tp = lax.axis_index("ep"), lax.axis_index("tp")
    z, y = ep // COLS, ep % COLS
    x, core = tp // CORES, tp % CORES
    rows, width = tokens.shape
    experts = w_gate.shape[0]
    hid = w_gate.shape[1]
    shid = s_gate.shape[0]
    cuts = cuts_of(width)
    pieces = len(cuts)
    split = hl0.shape[-1] // 2
    last = experts - 1
    mate = (ep, x * CORES + 1 - core)
    across = (ep, (1 - x) * CORES + core)
    diagonal = (ep, (1 - x) * CORES + 1 - core)
    beside = (z * COLS + 1 - y, tp)
    along = [None] + [(flip(z, r, n_rows_z) * COLS + y, tp) for r in range(1, n_rows_z)]
    at_end = jnp.where(z % 3 == 0, 1, 0)
    inner = at_end == 0
    order = [0, 1, 3 - at_end, 2 + at_end]

    barrier = pltpu.get_barrier_semaphore()
    peers = [mate, across, diagonal, beside] + along[1:]
    for peer in peers:
        pl.semaphore_signal(barrier, inc=1, device_id=peer, device_id_type=MESH)

    def local(src, dst, sem):
        c = pltpu.make_async_copy(src, dst, sem)
        c.start()
        return c

    inputs = [
        local(src, dst, in_sem.at[i])
        for i, (src, dst) in enumerate(
            (
                (tokens_in, tokens),
                (gain_in, gain),
                (ids_in, ids),
                (dropped_in, dropped),
                (gates_in, gates),
            )
        )
    ]
    chunks = []

    def add_chunk(source, e, m, start, size):
        rows_cut = pl.ds(start, size)
        chunks.append((source.at[e, rows_cut], lambda s: gu.at[e, m, s, rows_cut]))

    for e in range(experts):
        add_chunk(w_gate, e, 0, 0, hid)
        if e < last:
            add_chunk(w_up, e, 1, 0, hid)
        else:
            add_chunk(w_up, e, 1, 0, split)
            add_chunk(w_up, e, 1, split, hid - split)
    first_down = len(chunks)
    for cut in cuts:
        chunks.append(
            (w_down.at[:, :, cut], functools.partial(lambda cut, s: db.at[:, s, :, cut], cut))
        )
    n = len(chunks)

    def whole(s):
        return [(w_gate, gu.at[:, 0, s]), (w_up, gu.at[:, 1, s]), (w_down, db.at[:, s])]

    own = [local(src, dst, own_sem.at[i]) for i, (src, dst) in enumerate(whole(0))]
    shared_in = [local(s_gate, sg, own_sem.at[3]), local(s_up, su, own_sem.at[4])]
    who = [tp, mate[1], across[1], diagonal[1]]
    for s in range(4):
        local(
            s_down.at[pl.ds(pl.multiple_of(who[s] * shid, 16), shid), :],
            sd.at[pl.ds(s * shid, shid)],
            own_sem.at[5],
        )

    pl.semaphore_wait(barrier, len(peers))
    def copy_to(src, dst, ssem, rsem, peer):
        return pltpu.make_async_remote_copy(
            src_ref=src,
            dst_ref=dst,
            send_sem=ssem,
            recv_sem=rsem,
            device_id=peer,
            device_id_type=MESH,
        )

    def remote(src, dst, ssem, rsem, peer):
        c = copy_to(src, dst, ssem, rsem, peer)
        c.start()
        return c

    def group(k):
        return 0 if k < first_down else 1

    far = [
        copy_to(source, place(2), far_send.at[group(k)], far_recv.at[k], across)
        for k, (source, place) in enumerate(chunks)
    ]
    late = range(first_down + 1, n)
    for k in [*range(first_down - 1), first_down, first_down - 1]:
        far[k].start()

    @pl.when(core == 0)
    def _():
        for k in late:
            far[k].start()

    near = [
        remote(src, dst, near_send.at[i], near_recv.at[i], mate)
        for i, (src, dst) in enumerate(whole(1))
    ]

    for c in inputs:
        c.wait()
    values = tokens[...].astype(jnp.float32)
    scale = lax.rsqrt(jnp.mean(values * values, axis=-1, keepdims=True) + 1e-06)
    xb[0, 0] = (values * scale * gain[...]).astype(jnp.bfloat16)
    table = jnp.zeros(wtb.shape[2:], jnp.float32)
    rows_of = lax.broadcasted_iota(jnp.int32, wtb.shape[2:], 0)
    for k in range(ids.shape[0]):
        hit = (ids[k : k + 1, :] == rows_of) & (dropped[k : k + 1, :] == 0)
        table = table + jnp.where(hit, gates[k : k + 1, :], 0.0)
    wtb[0, 0] = table

    half = rows // 2
    parts = 3

    def part(i, side, slot):
        if i == 0:
            return wtb.at[side, slot]
        return xb.at[side, slot, pl.ds((i - 1) * half, half)]

    routes = [(0, 1, 1), (0, 3, 3), (1, 2, 3), (3, 2, 1), (2, 3, 1)]
    hops = [
        [
            copy_to(
                part(i, 0, src),
                part(i, 0, dst),
                z_send.at[min(k, 1), min(i, 1)],
                z_recv.at[i, dst - 1],
                along[by],
            )
            for i in range(parts)
        ]
        for k, (src, dst, by) in enumerate(routes)
    ]

    def arrived(i, slot):
        copy_to(
            part(i, 0, 0), part(i, 0, slot), z_send.at[0, 0], z_recv.at[i, slot - 1], along[1]
        ).wait_recv()

    def to_side(k, i):
        slot = order[k]
        m = min(i, 1)
        remote(part(i, 0, slot), part(i, 1, slot), y_send.at[m], y_recv.at[m, k], beside)

    def from_side(k):
        for m, ref in enumerate((wtb, xb)):
            slot = ref.at[1, order[k]]
            copy_to(slot, slot, y_send.at[m], y_recv.at[m, k], beside).wait_recv()

    for i in range(parts):
        hops[0][i].start()

    @pl.when(inner)
    def _():
        for i in range(parts):
            hops[1][i].start()

    for i in range(parts):
        to_side(0, i)
    share_near = remote(xb.at[0, 0], sb.at[1], t_send, t_recv.at[0], mate)
    share_far = copy_to(xb.at[0, 0], sb.at[2], t_send, t_recv.at[1], across)

    @pl.when(core == 0)
    def _():
        share_far.start()

    passed = {}

    def pass_on(k):
        far[k].wait_recv()
        place = chunks[k][1]
        passed[k] = remote(place(2), place(3), pass_send.at[group(k)], pass_recv.at[k], mate)

    def column(side, r, e):
        line = jnp.sum(
            jnp.where(rows_of == ep * experts + e, wtb[side, r], 0.0), axis=0, keepdims=True
        )
        return jnp.transpose(jnp.broadcast_to(line, (rows, rows)))[:, 0:1]

    def both_sides(r):
        return jnp.concatenate([xb[0, r], xb[1, r]], axis=0)

    def two_rows(side, q):
        return xb[side, pl.ds(2 * q, 2)].reshape(2 * rows, width)

    def matrix(e, m, pair, start, size):
        picked = gu[e, m, 2 * pair : 2 * pair + 2, start : start + size]
        return picked.reshape(2 * size, width)

    def activate(g, u, r, e):
        weight = jnp.concatenate([column(0, r, e), column(1, r, e)], axis=0)
        return (g * jax.nn.sigmoid(g) * u * weight).astype(jnp.bfloat16)

    def hidden(r, pair, e):
        left = both_sides(r)
        g = dot(left, matrix(e, 0, pair, 0, hid), NT)
        u = dot(left, matrix(e, 1, pair, 0, hid), NT)
        h = activate(g, u, r, e)
        hb[0, e * 2 + pair, r] = h[:rows]
        hb[1, e * 2 + pair, r] = h[rows:]

    def near_hidden(k):
        def body(e, carry):
            hidden(order[k], 0, e)
            return carry

        lax.fori_loop(0, experts, body, 0)

    def far_hidden(first, count):
        def body(i, carry):
            r = i
            for k in range(1, n_rows_z):
                r = jnp.where(i == k, order[k], r)
            hidden(r, 1, 0)
            return carry

        lax.fori_loop(first, first + count, body, 0)

    def last_gate():
        def body(i, carry):
            left = two_rows(i // 2, i % 2)
            ga0[i] = dot(left, matrix(last, 0, 1, 0, split), NT)
            ga1[i] = dot(left, matrix(last, 0, 1, split, hid - split), NT)
            return carry

        lax.fori_loop(0, n_rows_z, body, 0)

    def last_up(stored, start, size, place, side):
        def body(q, carry):
            u = dot(two_rows(side, q), matrix(last, 1, 1, start, size), NT)
            g = stored[2 * side + q]
            weight = [column(side, 2 * q + i, last) for i in range(2)]
            h = g * jax.nn.sigmoid(g) * u * jnp.concatenate(weight, axis=0)
            place[side, pl.ds(2 * q, 2)] = h.astype(jnp.bfloat16).reshape(2, rows, 2 * size)
            return carry

        lax.fori_loop(0, n_rows_z // 2, body, 0)

    def shared_hidden(pair):
        left = xb[0, 0] if pair == 0 else sb[2]
        left = jnp.concatenate([left, sb[2 * pair + 1]], axis=0)
        g = dot(left, sg[...], NT)
        u = dot(left, su[...], NT)
        h = (g * jax.nn.sigmoid(g) * u).astype(jnp.bfloat16)
        sh[2 * pair] = h[:rows]
        sh[2 * pair + 1] = h[rows:]

    for i in range(2):
        own[i].wait()
        near[i].wait_recv()
    for i in range(parts):
        arrived(i, 1)
        to_side(1, i)

        @pl.when(inner)
        def _(i=i):
            hops[2][i].start()
            arrived(i, 3)
            hops[3][i].start()

    from_side(0)
    near_hidden(0)
    for c in shared_in:
        c.wait()
    share_near.wait_recv()
    shared_hidden(0)
    share_back = remote(sh.at[1], whid.at[1], h_send, h_recv.at[0], mate)
    pass_on(0)
    for i in range(parts):

        @pl.when(inner)
        def _(i=i):
            arrived(i, 2)
            hops[4][i].start()

        @pl.when(at_end == 1)
        def _(i=i):
            arrived(i, 2)

        to_side(2, i)
    from_side(1)
    near_hidden(1)
    for i in range(parts):

        @pl.when(at_end == 1)
        def _(i=i):
            arrived(i, 3)

        to_side(3, i)
        if i == 1:
            pass_on(1)
            passed[0].wait_recv()
            passed[1].wait_recv()
            far_hidden(0, 2)
    from_side(2)
    near_hidden(2)
    far_hidden(2, 1)
    from_side(3)
    near_hidden(3)
    far_hidden(3, 1)
    pass_on(2)
    passed[2].wait_recv()
    last_gate()
    pass_on(3)
    passed[3].wait_recv()
    for side in range(COLS):
        last_up(ga0, 0, split, hl0, side)
    pass_on(first_down)
    pass_on(first_down - 1)

    @pl.when(core == 0)
    def _():
        pl.semaphore_signal(go, inc=1, device_id=mate, device_id_type=MESH)

    @pl.when(core == 1)
    def _():
        pl.semaphore_wait(go, 1)
        for k in late:
            far[k].start()
        share_far.start()

    passed[first_down - 1].wait_recv()
    last_up(ga1, split, hid - split, hl1, 1)

    def down(c, side):
        cut = cuts[c]
        piece = cut.size

        def body(q, carry):
            total = None

            def add(total, left, e, pair, start, size):
                left = left.reshape(2 * rows, 2 * size)
                right = db[e, 2 * pair : 2 * pair + 2, start : start + size, cut]
                part = dot(left, right.reshape(2 * size, piece), NN)
                return part if total is None else total + part

            two = pl.ds(2 * q, 2)
            for e in range(experts):
                for pair in range(2):
                    if 2 * e + pair < 2 * experts - 1:
                        total = add(total, hb[side, 2 * e + pair, two], e, pair, 0, hid)
            total = add(total, hl0[side, two], last, 1, 0, split)
            total = add(total, hl1[side, two], last, 1, split, hid - split)
            total = total.reshape(2, rows, piece)
            if side:
                ysend[two, :, cut] = total.astype(jnp.bfloat16)
            else:
                ypart[two, :, cut] = total
            return carry

        lax.fori_loop(0, n_rows_z // 2, body, 0)

    end = pieces - 1

    def side_leg(c, r):
        sem = ry_recv.at[c + (n_rows_z - 1 - r if c == end else 0)]
        span = r if c == end else pl.ds(0, n_rows_z)
        return copy_to(
            ysend.at[span, :, cuts[c]], yrecv.at[span, :, cuts[c]], ry_send, sem, beside
        )

    def send_side(c):
        for r in range(n_rows_z - 1, -1, -1) if c == end else (0,):
            side_leg(c, r).start()

    def block(c, r, extra=None):
        cut = cuts[c]
        total = ypart[r, :, cut] + yrecv[r, :, cut].astype(jnp.float32)
        if extra is not None:
            total = total + zrecv[extra, :, cut].astype(jnp.float32)
        zsend[r, :, cut] = total.astype(jnp.bfloat16)

    def leg(c, r, slot, by, sem):
        return copy_to(
            zsend.at[r, :, cuts[c]], zrecv.at[slot, :, cuts[c]], rz_send, sem, along[by]
        )

    def join_sem(c, slot):
        return rz_join.at[c + (1 if c == end and slot == 2 else 0)]

    def last_sem(c):
        return rz_recv.at[max(c - end + 2, 0)]

    def turn(c):
        if c < end:
            side_leg(c, 0).wait_recv()

        @pl.when(at_end == 1)
        def _():
            for r, slot in ((3, 0), (2, 2), (1, 1)):
                if c == end:
                    side_leg(c, r).wait_recv()
                block(c, r)
                leg(c, r, slot, 1, join_sem(c, slot) if r > 1 else last_sem(c)).start()

        @pl.when(inner)
        def _():
            if c == end:
                for r in (3, 2, 1):
                    side_leg(c, r).wait_recv()
            block(c, 1)
            leg(c, 1, 1, 1, last_sem(c)).start()

        if c == end:
            side_leg(c, 0).wait_recv()

    def join(c):
        @pl.when(inner)
        def _():
            if c < end:
                both = zrecv.at[pl.ds(0, 2), :, cuts[c]]
                copy_to(both, both, rz_send, join_sem(c, 0), along[1]).wait_recv()
            for r, slot in ((2, 0), (3, 2)):
                if c == end:
                    leg(c, 1, slot, 1, join_sem(c, slot)).wait_recv()
                block(c, r, slot)
                leg(c, r, r, r, last_sem(c)).start()

    def base(first, stop, c):
        cut = cuts[c]
        total = ypart[0, :, cut]
        if first == 0:
            total = total + tokens[:, cut].astype(jnp.float32)
        for s in range(first, stop):
            left = sh[0] if s == 0 else whid[s]
            total = total + dot(left, sd[s * shid : (s + 1) * shid, cut], NN)
        ypart[0, :, cut] = total

    def landed(first, stop):
        start = cuts[first].start
        span = pl.ds(start, cuts[stop - 1].start + cuts[stop - 1].size - start)
        both = zrecv.at[pl.ds(0, 2), :, span]
        copy_to(both, both, rz_send, last_sem(first), along[1]).wait_recv()

    def final(c):
        cut = cuts[c]
        total = ypart[0, :, cut] + yrecv[0, :, cut].astype(jnp.float32)
        for slot in (1, order[2]):
            total = total + zrecv[slot, :, cut].astype(jnp.float32)
        out[:, cut] = total.astype(out.dtype)
        local(out.at[:, cut], result.at[:, cut], out_sem)

    own[2].wait()
    near[2].wait_recv()
    for c in range(pieces):
        k = first_down + c
        if k not in passed:
            pass_on(k)
        passed[k].wait_recv()
        down(c, 1)
        send_side(c)
        if c == 0:
            last_up(ga1, split, hid - split, hl1, 0)
        down(c, 0)
        if c == 0:
            pltpu.make_async_copy(s_down, sd, own_sem.at[5]).wait()
            share_back.wait_recv()
        base(0, 2, c)
        if c == end:
            share_far.wait_recv()
            share_on = remote(sb.at[2], sb.at[3], t_send, t_recv.at[2], mate)
        if 2 < c < end:
            pass_on(k + 1)
        if c > 2:
            join(c - 3)
        if c > 1:
            turn(c - 2)

    share_on.wait_recv()
    shared_hidden(1)
    remote(sh.at[2], whid.at[2], h_send, h_recv.at[1], across)
    remote(sh.at[3], whid.at[3], h_send, h_recv.at[1], diagonal)
    turn(end - 1)
    join(end - 2)
    turn(end)
    join(end - 1)
    join(end)
    both_back = whid.at[pl.ds(2, 2)]
    copy_to(both_back, both_back, h_send, h_recv.at[1], across).wait_recv()
    for c in range(pieces):
        base(2, 4, c)
    landed(0, end - 1)
    for c in range(end - 1):
        final(c)
    for c in (end - 1, end):
        landed(c, c + 1)
        final(c)

    def drain(ref, sem):
        copy_to(ref, ref, sem, near_recv.at[0], mate).wait_send()

    for c in near:
        c.wait_send()
    for sems in (far_send, pass_send):
        drain(gu.at[:, :, 2], sems.at[0])
        drain(db.at[:, 2], sems.at[1])
    for m, ref in enumerate((wtb, xb)):
        drain(ref.at[0, 0], z_send.at[0, m])
        drain(ref.at[0], y_send.at[m])
    drain(sb.at[pl.ds(0, 3)], t_send)
    drain(sh.at[pl.ds(0, 3)], h_send)
    drain(ysend, ry_send)
    drain(zsend.at[pl.ds(1, 3)], rz_send)

    @pl.when(inner)
    def _():
        for m, ref in enumerate((wtb, xb)):
            drain(ref.at[0], z_send.at[1, m])

    pltpu.make_async_copy(out, result, out_sem).wait()


def scratch_of(n_rows_z, rows, top, width, n_experts, experts, hid, shid):
    bf, f4 = jnp.bfloat16, jnp.float32
    pieces = len(cuts_of(width))
    lines = n_experts
    split = hid - hid // 32 * 16
    pad = lambda v: -(-v // 128) * 128
    shapes = [
        ((rows, width), bf),
        ((1, width), f4),
        ((top, rows), jnp.int32),
        ((top, rows), jnp.int32),
        ((top, rows), f4),
        ((rows, width), bf),
        ((COLS, n_rows_z, rows, width), bf),
        ((COLS, n_rows_z, lines, rows), f4),
        ((experts, 2, 4, hid, width), bf),
        ((n_rows_z, 2 * rows, 2 * split), f4),
        ((n_rows_z, 2 * rows, 2 * (hid - split)), f4),
        ((experts, 4, hid, width), bf),
        ((COLS, 2 * experts - 1, n_rows_z, rows, 2 * hid), bf),
        ((COLS, n_rows_z, rows, 2 * split), bf),
        ((COLS, n_rows_z, rows, 2 * (hid - split)), bf),
        ((4, rows, width), bf),
        ((shid, width), bf),
        ((shid, width), bf),
        ((4 * shid, width), bf),
        ((4, rows, shid), bf),
        ((4, rows, shid), bf),
        ((n_rows_z, rows, width), bf),
        ((n_rows_z, rows, width), bf),
        ((n_rows_z, rows, width), f4),
        ((n_rows_z, rows, width), bf),
        ((n_rows_z, rows, width), bf),
    ]
    total = 0
    for dims, kind in shapes:
        size = pad(dims[-1]) * jnp.dtype(kind).itemsize
        for d in dims[:-1]:
            size *= d
        total += size
    n = 2 * experts + 1 + pieces
    dma = pltpu.SemaphoreType.DMA
    one = pltpu.SemaphoreType.DMA
    sems = [dma((6,)), dma((3,)), dma((3,)), dma((2,)), dma((n,)), dma((2,)), dma((n,))]
    sems += [dma((2, 2)), dma((3, n_rows_z - 1)), dma((2,)), dma((2, n_rows_z))]
    sems += [one, dma((3,)), one, dma((2,))]
    sems += [one, dma((pieces + n_rows_z - 1,)), one, dma((pieces + 1,)), dma((3,))]
    sems += [pltpu.SemaphoreType.REGULAR, dma((5,)), one]
    return [pltpu.VMEM(d, k) for d, k in shapes] + sems, total


def fused(n_rows_z, scratch, tokens, gain, ids, slot, dropped, gates, wg, wu, wd, sg, su, sd):
    hbm = pl.BlockSpec(memory_space=pl.ANY)
    return pl.pallas_call(
        functools.partial(layer_kernel, n_rows_z),
        out_shape=jax.ShapeDtypeStruct(tokens.shape, tokens.dtype),
        in_specs=[hbm] * 11,
        out_specs=hbm,
        scratch_shapes=scratch,
        compiler_params=pltpu.CompilerParams(
            collective_id=0, has_side_effects=True, vmem_limit_bytes=VMEM_BYTES
        ),
        name="moe_layer",
    )(
        tokens,
        gain[None, :],
        ids.T,
        dropped.T,
        gates.T,
        wg.transpose(0, 2, 1),
        wu.transpose(0, 2, 1),
        wd.transpose(0, 2, 1),
        sg.T,
        su.T,
        sd,
    )


TOP = 6
EXP_DEV = 2
TOK_DEV = 128


norm_eps = 1e-06


def swiglu(left, right):
    return jax.nn.silu(left) * right


def on_device(
    tokens,
    norm_gain,
    expert_ids,
    slot_index,
    dropped,
    gates,
    w_gate,
    w_up,
    w_down,
    shared_gate,
    shared_up,
    shared_down,
):
    n_expert_groups = lax.axis_size("ep")
    experts = EXP_DEV * n_expert_groups
    capacity = TOK_DEV * TOP * 4 // (experts * 3)
    model_width = tokens.shape[1]
    local_rows = tokens.shape[0]
    values = tokens.astype(jnp.float32)
    scale = lax.rsqrt(jnp.mean(values * values, axis=-1, keepdims=True) + norm_eps)
    normed = (values * scale * norm_gain).astype(jnp.bfloat16)
    destination_position = expert_ids * capacity + slot_index
    kept_pair = dropped == 0
    matrix_breadth = lax.iota(jnp.int32, experts * capacity)
    matches = (destination_position[:, :, None] == matrix_breadth[None, None, :]) & kept_pair[
        :, :, None
    ]
    dispatch_table = jnp.any(matches, axis=1).astype(jnp.bfloat16)
    outgoing = lax.dot_general(
        dispatch_table, normed, (((0,), (0,)), ((), ())), preferred_element_type=jnp.float32
    ).astype(jnp.bfloat16)
    boxes = outgoing.reshape(n_expert_groups, EXP_DEV, capacity, model_width)
    received = lax.all_to_all(boxes, "ep", split_axis=0, concat_axis=0, tiled=True)
    gate_all = lax.all_gather(w_gate, "tp", axis=2, tiled=True)
    up_all = lax.all_gather(w_up, "tp", axis=2, tiled=True)
    down_all = lax.all_gather(w_down, "tp", axis=2, tiled=True)
    gate_act = jnp.einsum("iecd,edf->iecf", received, gate_all, preferred_element_type=jnp.float32)
    up_act = jnp.einsum("iecd,edf->iecf", received, up_all, preferred_element_type=jnp.float32)
    hidden = swiglu(gate_act, up_act).astype(jnp.bfloat16)
    expert_out = jnp.einsum(
        "iecf,edf->iecd", hidden, down_all, preferred_element_type=jnp.float32
    ).astype(jnp.bfloat16)
    returned_output = lax.all_to_all(expert_out, "ep", split_axis=0, concat_axis=0, tiled=True)
    returned_rows = returned_output.reshape(experts * capacity, model_width)
    shard_piece = lax.all_gather(normed, "tp", axis=0, tiled=True)
    gate_act = jnp.dot(shard_piece, shared_gate, preferred_element_type=jnp.float32)
    up_act = jnp.dot(shard_piece, shared_up, preferred_element_type=jnp.float32)
    partial_hidden = swiglu(gate_act, up_act).astype(jnp.bfloat16)
    whole_hidden = lax.all_to_all(partial_hidden, "tp", split_axis=0, concat_axis=1, tiled=True)
    shared_out = jnp.dot(whole_hidden, shared_down, preferred_element_type=jnp.float32)
    safe_target = jnp.where(kept_pair, destination_position, 0)
    picked = jnp.take(returned_rows, safe_target.reshape(-1), axis=0).reshape(
        local_rows, TOP, model_width
    )
    kept_weights = jnp.where(kept_pair, gates, jnp.float32(0.0))
    routed = jnp.sum(picked.astype(jnp.float32) * kept_weights[:, :, None], axis=1)
    return (values + shared_out + routed).astype(jnp.bfloat16)


def solution(mesh):
    ep, tp = mesh.shape["ep"], mesh.shape["tp"]
    placed = (
        P(("ep", "tp"), None),
        P(),
        P(("ep", "tp"), None),
        P(("ep", "tp"), None),
        P(("ep", "tp"), None),
        P(("ep", "tp"), None),
        P("ep", None, "tp"),
        P("ep", None, "tp"),
        P("ep", None, "tp"),
        P(None, "tp"),
        P(None, "tp"),
        P(),
    )

    def layer(*args):
        tokens, w_gate, shared_gate = args[0], args[6], args[9]
        n_rows_z = ep // COLS
        scratch, size = scratch_of(
            n_rows_z,
            tokens.shape[0],
            args[2].shape[1],
            tokens.shape[1],
            ep * w_gate.shape[0],
            w_gate.shape[0],
            w_gate.shape[2],
            shared_gate.shape[1],
        )
        spare = 8 * 1024 * 1024
        if tp == 2 * CORES and n_rows_z == 4 and w_gate.shape[0] == 2 and size + spare < VMEM_BYTES:
            return fused(n_rows_z, scratch, *args)
        return on_device(*args)

    return jax.shard_map(
        layer, mesh=mesh, in_specs=placed, out_specs=P(("ep", "tp"), None), check_vma=False
    )
```

```python
import functools

import jax
import jax.numpy as jnp
from jax import lax
from jax.experimental import pallas as pl
from jax.experimental.pallas import tpu as pltpu
from jax.sharding import PartitionSpec as P

MESH = pl.DeviceIdType.MESH
CORES = 2
COLS = 2
VMEM_BYTES = 62 * 1024 * 1024
LANES = 128
SWING = 3

NT = (((1,), (1,)), ((), ()))
NN = (((1,), (0,)), ((), ()))


def dot(a, b, dims):
    return lax.dot_general(a, b, dims, preferred_element_type=jnp.float32)


def flip(index, mask, size):
    out, bit = 0, 1
    while bit < size:
        digit = (index // bit) % 2
        out = out + (1 - digit if mask & bit else digit) * bit
        bit *= 2
    return out


def cuts_of(width):
    inside = width - 6 * LANES
    sizes = [LANES] * 2 + [2 * LANES] * (inside // (2 * LANES)) + [LANES] * 4
    starts = [sum(sizes[:i]) for i in range(len(sizes))]
    return [pl.ds(*cut) for cut in zip(starts, sizes)]


def layer_kernel(
    n_rows_z,
    tokens_in,
    gain_in,
    ids_in,
    dropped_in,
    gates_in,
    w_gate,
    w_up,
    w_down,
    s_gate,
    s_up,
    s_down,
    result,
    tokens,
    gain,
    ids,
    dropped,
    gates,
    out,
    xb,
    wtb,
    gu,
    ga0,
    ga1,
    db,
    hb,
    hl0,
    hl1,
    sb,
    sg,
    su,
    sd,
    sh,
    whid,
    ysend,
    yrecv,
    ypart,
    zsend,
    zrecv,
    zsend2,
    zrecv2,
    own_sem,
    near_send,
    near_recv,
    far_send,
    far_recv,
    pass_send,
    pass_recv,
    z_send,
    z_recv,
    y_send,
    y_recv,
    t_send,
    t_recv,
    h_send,
    h_recv,
    ry_send,
    ry_recv,
    rz_send,
    rz_join,
    rz_recv,
    sw_send,
    sw_join,
    sw_recv,
    go,
    in_sem,
    out_sem,
):
    ep, tp = lax.axis_index("ep"), lax.axis_index("tp")
    z, y = ep // COLS, ep % COLS
    x, core = tp // CORES, tp % CORES
    rows, width = tokens.shape
    experts = w_gate.shape[0]
    hid = w_gate.shape[1]
    shid = s_gate.shape[0]
    cuts = cuts_of(width)
    pieces = len(cuts)
    split = hl0.shape[-1] // 2
    last = experts - 1
    mate = (ep, x * CORES + 1 - core)
    across = (ep, (1 - x) * CORES + core)
    diagonal = (ep, (1 - x) * CORES + 1 - core)
    beside = (z * COLS + 1 - y, tp)
    along = [None] + [(flip(z, r, n_rows_z) * COLS + y, tp) for r in range(1, n_rows_z)]
    at_end = jnp.where(z % 3 == 0, 1, 0)
    inner = at_end == 0
    order = [0, 1, 3 - at_end, 2 + at_end]

    barrier = pltpu.get_barrier_semaphore()
    peers = [mate, across, diagonal, beside] + along[1:]
    for peer in peers:
        pl.semaphore_signal(barrier, inc=1, device_id=peer, device_id_type=MESH)

    def local(src, dst, sem):
        c = pltpu.make_async_copy(src, dst, sem)
        c.start()
        return c

    inputs = [
        local(src, dst, in_sem.at[i])
        for i, (src, dst) in enumerate(
            (
                (tokens_in, tokens),
                (gain_in, gain),
                (ids_in, ids),
                (dropped_in, dropped),
                (gates_in, gates),
            )
        )
    ]
    chunks = []

    def add_chunk(source, e, m, start, size):
        rows_cut = pl.ds(start, size)
        chunks.append((source.at[e, rows_cut], lambda s: gu.at[e, m, s, rows_cut]))

    for e in range(experts):
        add_chunk(w_gate, e, 0, 0, hid)
        if e < last:
            add_chunk(w_up, e, 1, 0, hid)
        else:
            add_chunk(w_up, e, 1, 0, split)
            add_chunk(w_up, e, 1, split, hid - split)
    first_down = len(chunks)
    for cut in cuts:
        chunks.append(
            (w_down.at[:, :, cut], functools.partial(lambda cut, s: db.at[:, s, :, cut], cut))
        )
    n = len(chunks)

    def whole(s):
        return [(w_gate, gu.at[:, 0, s]), (w_up, gu.at[:, 1, s]), (w_down, db.at[:, s])]

    own = [local(src, dst, own_sem.at[i]) for i, (src, dst) in enumerate(whole(0))]
    shared_in = [local(s_gate, sg, own_sem.at[3]), local(s_up, su, own_sem.at[4])]
    who = [tp, mate[1], across[1], diagonal[1]]
    for s in range(4):
        local(
            s_down.at[pl.ds(pl.multiple_of(who[s] * shid, 16), shid), :],
            sd.at[pl.ds(s * shid, shid)],
            own_sem.at[5],
        )

    pl.semaphore_wait(barrier, len(peers))
    def copy_to(src, dst, ssem, rsem, peer):
        return pltpu.make_async_remote_copy(
            src_ref=src,
            dst_ref=dst,
            send_sem=ssem,
            recv_sem=rsem,
            device_id=peer,
            device_id_type=MESH,
        )

    def remote(src, dst, ssem, rsem, peer):
        c = copy_to(src, dst, ssem, rsem, peer)
        c.start()
        return c

    def group(k):
        return 0 if k < first_down else 1

    far = [
        copy_to(source, place(2), far_send.at[group(k)], far_recv.at[k], across)
        for k, (source, place) in enumerate(chunks)
    ]
    late = range(first_down + 2, n)
    for k in [*range(first_down - 1), first_down, first_down - 1, first_down + 1]:
        far[k].start()

    @pl.when(core == 0)
    def _():
        for k in late:
            far[k].start()

    near = [
        remote(src, dst, near_send.at[i], near_recv.at[i], mate)
        for i, (src, dst) in enumerate(whole(1))
    ]

    for c in inputs:
        c.wait()
    values = tokens[...].astype(jnp.float32)
    scale = lax.rsqrt(jnp.mean(values * values, axis=-1, keepdims=True) + 1e-06)
    xb[0, 0] = (values * scale * gain[...]).astype(jnp.bfloat16)
    table = jnp.zeros(wtb.shape[2:], jnp.float32)
    rows_of = lax.broadcasted_iota(jnp.int32, wtb.shape[2:], 0)
    for k in range(ids.shape[0]):
        hit = (ids[k : k + 1, :] == rows_of) & (dropped[k : k + 1, :] == 0)
        table = table + jnp.where(hit, gates[k : k + 1, :], 0.0)
    wtb[0, 0] = table

    half = rows // 2
    parts = 3

    def part(i, side, slot):
        if i == 0:
            return wtb.at[side, slot]
        return xb.at[side, slot, pl.ds((i - 1) * half, half)]

    routes = [(0, 1, 1), (0, 3, 3), (1, 2, 3), (3, 2, 1), (2, 3, 1)]
    hops = [
        [
            copy_to(
                part(i, 0, src),
                part(i, 0, dst),
                z_send.at[min(k, 1), min(i, 1)],
                z_recv.at[i, dst - 1],
                along[by],
            )
            for i in range(parts)
        ]
        for k, (src, dst, by) in enumerate(routes)
    ]

    def arrived(i, slot):
        copy_to(
            part(i, 0, 0), part(i, 0, slot), z_send.at[0, 0], z_recv.at[i, slot - 1], along[1]
        ).wait_recv()

    def to_side(k, i):
        slot = order[k]
        m = min(i, 1)
        remote(part(i, 0, slot), part(i, 1, slot), y_send.at[m], y_recv.at[m, k], beside)

    def from_side(k):
        for m, ref in enumerate((wtb, xb)):
            slot = ref.at[1, order[k]]
            copy_to(slot, slot, y_send.at[m], y_recv.at[m, k], beside).wait_recv()

    for i in range(parts):
        hops[0][i].start()

    @pl.when(inner)
    def _():
        for i in range(parts):
            hops[1][i].start()

    for i in range(parts):
        to_side(0, i)
    share_near = remote(xb.at[0, 0], sb.at[1], t_send, t_recv.at[0], mate)
    share_far = copy_to(xb.at[0, 0], sb.at[2], t_send, t_recv.at[1], across)

    @pl.when(core == 0)
    def _():
        share_far.start()

    passed = {}

    def pass_on(k):
        far[k].wait_recv()
        place = chunks[k][1]
        passed[k] = remote(place(2), place(3), pass_send.at[group(k)], pass_recv.at[k], mate)

    def column(side, r, e):
        line = jnp.sum(
            jnp.where(rows_of == ep * experts + e, wtb[side, r], 0.0), axis=0, keepdims=True
        )
        return jnp.transpose(jnp.broadcast_to(line, (rows, rows)))[:, 0:1]

    def both_sides(r):
        return jnp.concatenate([xb[0, r], xb[1, r]], axis=0)

    def two_rows(side, q):
        return xb[side, pl.ds(2 * q, 2)].reshape(2 * rows, width)

    def matrix(e, m, pair, start, size):
        picked = gu[e, m, 2 * pair : 2 * pair + 2, start : start + size]
        return picked.reshape(2 * size, width)

    def activate(g, u, r, e):
        weight = jnp.concatenate([column(0, r, e), column(1, r, e)], axis=0)
        return (g * jax.nn.sigmoid(g) * u * weight).astype(jnp.bfloat16)

    def hidden(r, pair, e):
        left = both_sides(r)
        g = dot(left, matrix(e, 0, pair, 0, hid), NT)
        u = dot(left, matrix(e, 1, pair, 0, hid), NT)
        h = activate(g, u, r, e)
        hb[0, e * 2 + pair, r] = h[:rows]
        hb[1, e * 2 + pair, r] = h[rows:]

    def near_hidden(k):
        def body(e, carry):
            hidden(order[k], 0, e)
            return carry

        lax.fori_loop(0, experts, body, 0)

    def far_hidden(first, count):
        def body(i, carry):
            r = i
            for k in range(1, n_rows_z):
                r = jnp.where(i == k, order[k], r)
            hidden(r, 1, 0)
            return carry

        lax.fori_loop(first, first + count, body, 0)

    def last_gate():
        def body(i, carry):
            left = two_rows(i // 2, i % 2)
            ga0[i] = dot(left, matrix(last, 0, 1, 0, split), NT)
            ga1[i] = dot(left, matrix(last, 0, 1, split, hid - split), NT)
            return carry

        lax.fori_loop(0, n_rows_z, body, 0)

    def last_up(stored, start, size, place, side):
        def body(q, carry):
            u = dot(two_rows(side, q), matrix(last, 1, 1, start, size), NT)
            g = stored[2 * side + q]
            weight = [column(side, 2 * q + i, last) for i in range(2)]
            h = g * jax.nn.sigmoid(g) * u * jnp.concatenate(weight, axis=0)
            place[side, pl.ds(2 * q, 2)] = h.astype(jnp.bfloat16).reshape(2, rows, 2 * size)
            return carry

        lax.fori_loop(0, n_rows_z // 2, body, 0)

    def shared_act(left):
        g = dot(left, sg[...], NT)
        u = dot(left, su[...], NT)
        return (g * jax.nn.sigmoid(g) * u).astype(jnp.bfloat16)

    def shared_hidden():
        h = shared_act(jnp.concatenate([xb[0, 0], sb[1]], axis=0))
        sh[0] = h[:rows]
        sh[1] = h[rows:]

    for i in range(2):
        own[i].wait()
        near[i].wait_recv()
    for i in range(parts):
        arrived(i, 1)
        to_side(1, i)

        @pl.when(inner)
        def _(i=i):
            hops[2][i].start()
            arrived(i, 3)
            hops[3][i].start()

    from_side(0)
    near_hidden(0)
    for c in shared_in:
        c.wait()
    share_near.wait_recv()
    shared_hidden()
    share_back = remote(sh.at[1], whid.at[1], h_send, h_recv.at[0], mate)
    pass_on(0)
    for i in range(parts):

        @pl.when(inner)
        def _(i=i):
            arrived(i, 2)
            hops[4][i].start()

        @pl.when(at_end == 1)
        def _(i=i):
            arrived(i, 2)

        to_side(2, i)
    from_side(1)
    near_hidden(1)
    for i in range(parts):

        @pl.when(at_end == 1)
        def _(i=i):
            arrived(i, 3)

        to_side(3, i)
        if i == 1:
            pass_on(1)
            passed[0].wait_recv()
            passed[1].wait_recv()
            far_hidden(0, 2)
    from_side(2)
    near_hidden(2)
    far_hidden(2, 1)
    from_side(3)
    near_hidden(3)
    far_hidden(3, 1)
    pass_on(2)
    passed[2].wait_recv()
    last_gate()
    pass_on(3)
    passed[3].wait_recv()
    for side in range(COLS):
        last_up(ga0, 0, split, hl0, side)
    pass_on(first_down)
    pass_on(first_down - 1)

    @pl.when(core == 0)
    def _():
        pl.semaphore_signal(go, inc=1, device_id=mate, device_id_type=MESH)

    @pl.when(core == 1)
    def _():
        pl.semaphore_wait(go, 1)
        for k in late:
            far[k].start()
        share_far.start()

    passed[first_down - 1].wait_recv()
    last_up(ga1, split, hid - split, hl1, 1)

    def down(c, side):
        cut = cuts[c]
        piece = cut.size

        def body(q, carry):
            total = None

            def add(total, left, e, pair, start, size):
                left = left.reshape(2 * rows, 2 * size)
                right = db[e, 2 * pair : 2 * pair + 2, start : start + size, cut]
                part = dot(left, right.reshape(2 * size, piece), NN)
                return part if total is None else total + part

            two = pl.ds(2 * q, 2)
            for e in range(experts):
                for pair in range(2):
                    if 2 * e + pair < 2 * experts - 1:
                        total = add(total, hb[side, 2 * e + pair, two], e, pair, 0, hid)
            total = add(total, hl0[side, two], last, 1, 0, split)
            total = add(total, hl1[side, two], last, 1, split, hid - split)
            total = total.reshape(2, rows, piece)
            if side:
                ysend[two, :, cut] = total.astype(jnp.bfloat16)
            else:
                ypart[two, :, cut] = total
            return carry

        lax.fori_loop(0, n_rows_z // 2, body, 0)

    end = pieces - 1

    def side_leg(c, r):
        sem = ry_recv.at[c + (n_rows_z - 1 - r if c == end else 0)]
        span = r if c == end else pl.ds(0, n_rows_z)
        return copy_to(
            ysend.at[span, :, cuts[c]], yrecv.at[span, :, cuts[c]], ry_send, sem, beside
        )

    def send_side(c):
        for r in range(n_rows_z - 1, -1, -1) if c == end else (0,):
            side_leg(c, r).start()

    def block(c, r, extra=None):
        cut = cuts[c]
        total = ypart[r, :, cut] + yrecv[r, :, cut].astype(jnp.float32)
        if extra is not None:
            total = total + zrecv[extra, :, cut].astype(jnp.float32)
        zsend[r, :, cut] = total.astype(jnp.bfloat16)

    def leg(c, r, slot, by, sem):
        return copy_to(
            zsend.at[r, :, cuts[c]], zrecv.at[slot, :, cuts[c]], rz_send, sem, along[by]
        )

    def join_sem(c, slot):
        return rz_join.at[c + (1 if c == end and slot == 2 else 0)]

    def last_sem(c):
        return rz_recv.at[max(c - end + 2, 0)]

    def turn(c):
        if c < end:
            side_leg(c, 0).wait_recv()

        @pl.when(at_end == 1)
        def _():
            for r, slot in ((3, 0), (2, 2), (1, 1)):
                if c == end:
                    side_leg(c, r).wait_recv()
                block(c, r)
                leg(c, r, slot, 1, join_sem(c, slot) if r > 1 else last_sem(c)).start()

        @pl.when(inner)
        def _():
            if c == end:
                for r in (3, 2, 1):
                    side_leg(c, r).wait_recv()
            block(c, 1)
            leg(c, 1, 1, 1, last_sem(c)).start()

        if c == end:
            side_leg(c, 0).wait_recv()

    def join(c):
        @pl.when(inner)
        def _():
            if c < end:
                both = zrecv.at[pl.ds(0, 2), :, cuts[c]]
                copy_to(both, both, rz_send, join_sem(c, 0), along[1]).wait_recv()
            for r, slot in ((2, 0), (3, 2)):
                if c == end:
                    leg(c, 1, slot, 1, join_sem(c, slot)).wait_recv()
                block(c, r, slot)
                leg(c, r, r, r, last_sem(c)).start()

    def swing_leg(src, slot, by, sem):
        return copy_to(src, zrecv2.at[slot], sw_send, sem, along[by])

    swing = cuts[SWING]

    def swing_out():
        def ahead(r, slot, sem, sem2):
            zsend[r, :, swing] = ypart[r, :, swing].astype(jnp.bfloat16)
            leg(SWING, r, slot, 1, sem).start()
            swing_leg(ysend.at[r, :, swing], slot, 1, sem2).start()

        @pl.when(at_end == 1)
        def _():
            for r, slot in ((3, 0), (2, 2)):
                ahead(r, slot, join_sem(SWING, slot), sw_join)
            ahead(1, 1, last_sem(SWING), sw_recv)

        @pl.when(inner)
        def _():
            ahead(1, 1, last_sem(SWING), sw_recv)

    def swing_join():
        @pl.when(inner)
        def _():
            both = zrecv.at[pl.ds(0, 2), :, swing]
            copy_to(both, both, rz_send, join_sem(SWING, 0), along[1]).wait_recv()
            both = zrecv2.at[pl.ds(0, 2)]
            copy_to(both, both, sw_send, sw_join, along[1]).wait_recv()
            for r, slot in ((2, 0), (3, 2)):
                total = ypart[r, :, swing] + zrecv[slot, :, swing].astype(jnp.float32)
                zsend[r, :, swing] = total.astype(jnp.bfloat16)
                leg(SWING, r, r, r, last_sem(SWING)).start()
                total = ysend[r, :, swing].astype(jnp.float32) + zrecv2[slot].astype(jnp.float32)
                zsend2[r] = total.astype(jnp.bfloat16)
                swing_leg(zsend2.at[r], r, r, sw_recv).start()

    def swing_side():
        return copy_to(zsend2.at[0], yrecv.at[0, :, swing], sw_send, ry_recv.at[SWING], beside)

    def swing_cross():
        both = zrecv2.at[pl.ds(0, 2)]
        copy_to(both, both, sw_send, sw_recv, along[1]).wait_recv()
        total = ysend[0, :, swing].astype(jnp.float32)
        for slot in (1, order[2]):
            total = total + zrecv2[slot].astype(jnp.float32)
        zsend2[0] = total.astype(jnp.bfloat16)
        swing_side().start()

    def base(first, stop, c):
        cut = cuts[c]
        total = ypart[0, :, cut]
        if first == 0:
            total = total + tokens[:, cut].astype(jnp.float32)
        for s in range(first, stop):
            left = sh[0] if s == 0 else whid[s]
            total = total + dot(left, sd[s * shid : (s + 1) * shid, cut], NN)
        ypart[0, :, cut] = total

    def landed(first, stop):
        start = cuts[first].start
        span = pl.ds(start, cuts[stop - 1].start + cuts[stop - 1].size - start)
        both = zrecv.at[pl.ds(0, 2), :, span]
        copy_to(both, both, rz_send, last_sem(first), along[1]).wait_recv()

    def final(c):
        cut = cuts[c]
        total = ypart[0, :, cut] + yrecv[0, :, cut].astype(jnp.float32)
        for slot in (1, order[2]):
            total = total + zrecv[slot, :, cut].astype(jnp.float32)
        out[:, cut] = total.astype(out.dtype)
        local(out.at[:, cut], result.at[:, cut], out_sem)

    steps = {
        2: [lambda: turn(0)],
        3: [swing_out, lambda: turn(1)],
        4: [lambda: turn(2), lambda: join(0)],
        6: [lambda: turn(4)],
        7: [swing_join],
        8: [lambda: join(1), lambda: turn(5)],
        end: [lambda: join(2), lambda: turn(6), swing_cross],
    }
    rest = [lambda: turn(7), lambda: join(4), lambda: turn(8), lambda: join(5)]
    steps[end] += rest
    own[2].wait()
    near[2].wait_recv()
    for c in range(pieces):
        k = first_down + c
        if k not in passed:
            pass_on(k)
        passed[k].wait_recv()
        down(c, 1)
        if c != SWING:
            send_side(c)
        if c == 0:
            pass_on(k + 1)
            last_up(ga1, split, hid - split, hl1, 0)
        down(c, 0)
        if c == 0:
            pltpu.make_async_copy(s_down, sd, own_sem.at[5]).wait()
            share_back.wait_recv()
        base(0, 2, c)
        if 0 < c < end:
            pass_on(k + 1)
        for step in steps.get(c, []):
            step()

    share_far.wait_recv()
    share_on = remote(sb.at[2], sb.at[3], t_send, t_recv.at[2], mate)
    sh[2] = shared_act(sb[2])
    remote(sh.at[2], whid.at[2], h_send, h_recv.at[1], across)
    share_on.wait_recv()
    sh[3] = shared_act(sb[3])
    remote(sh.at[3], whid.at[3], h_send, h_recv.at[1], diagonal)
    join(6)
    turn(end - 1)
    join(7)
    turn(end)
    for c in range(end - 2, end + 1):
        join(c)
    swing_side().wait_recv()
    both_back = whid.at[pl.ds(2, 2)]
    copy_to(both_back, both_back, h_send, h_recv.at[1], across).wait_recv()
    for c in range(pieces):
        base(2, 4, c)
    landed(0, end - 1)
    for c in range(end - 1):
        final(c)
    for c in (end - 1, end):
        landed(c, c + 1)
        final(c)

    def drain(ref, sem):
        copy_to(ref, ref, sem, near_recv.at[0], mate).wait_send()

    for c in near:
        c.wait_send()
    for sems in (far_send, pass_send):
        drain(gu.at[:, :, 2], sems.at[0])
        drain(db.at[:, 2], sems.at[1])
    for m, ref in enumerate((wtb, xb)):
        drain(ref.at[0, 0], z_send.at[0, m])
        drain(ref.at[0], y_send.at[m])
    drain(sb.at[pl.ds(0, 3)], t_send)
    drain(sh.at[pl.ds(0, 3)], h_send)
    drain(ysend.at[:, :, pl.ds(0, width - swing.size)], ry_send)
    drain(zsend2, sw_send)
    drain(zsend.at[pl.ds(1, 3)], rz_send)

    @pl.when(inner)
    def _():
        for m, ref in enumerate((wtb, xb)):
            drain(ref.at[0], z_send.at[1, m])

    pltpu.make_async_copy(out, result, out_sem).wait()


def scratch_of(n_rows_z, rows, top, width, n_experts, experts, hid, shid):
    bf, f4 = jnp.bfloat16, jnp.float32
    pieces = len(cuts_of(width))
    lines = n_experts
    split = hid - hid // 32 * 16
    pad = lambda v: -(-v // 128) * 128
    shapes = [
        ((rows, width), bf),
        ((1, width), f4),
        ((top, rows), jnp.int32),
        ((top, rows), jnp.int32),
        ((top, rows), f4),
        ((rows, width), bf),
        ((COLS, n_rows_z, rows, width), bf),
        ((COLS, n_rows_z, lines, rows), f4),
        ((experts, 2, 4, hid, width), bf),
        ((n_rows_z, 2 * rows, 2 * split), f4),
        ((n_rows_z, 2 * rows, 2 * (hid - split)), f4),
        ((experts, 4, hid, width), bf),
        ((COLS, 2 * experts - 1, n_rows_z, rows, 2 * hid), bf),
        ((COLS, n_rows_z, rows, 2 * split), bf),
        ((COLS, n_rows_z, rows, 2 * (hid - split)), bf),
        ((4, rows, width), bf),
        ((shid, width), bf),
        ((shid, width), bf),
        ((4 * shid, width), bf),
        ((4, rows, shid), bf),
        ((4, rows, shid), bf),
        ((n_rows_z, rows, width), bf),
        ((n_rows_z, rows, width), bf),
        ((n_rows_z, rows, width), f4),
        ((n_rows_z, rows, width), bf),
        ((n_rows_z, rows, width), bf),
        ((n_rows_z, rows, 2 * LANES), bf),
        ((n_rows_z, rows, 2 * LANES), bf),
    ]
    total = 0
    for dims, kind in shapes:
        size = pad(dims[-1]) * jnp.dtype(kind).itemsize
        for d in dims[:-1]:
            size *= d
        total += size
    n = 2 * experts + 1 + pieces
    dma = pltpu.SemaphoreType.DMA
    one = pltpu.SemaphoreType.DMA
    sems = [dma((6,)), dma((3,)), dma((3,)), dma((2,)), dma((n,)), dma((2,)), dma((n,))]
    sems += [dma((2, 2)), dma((3, n_rows_z - 1)), dma((2,)), dma((2, n_rows_z))]
    sems += [one, dma((3,)), one, dma((2,))]
    sems += [one, dma((pieces + n_rows_z - 1,)), one, dma((pieces + 1,)), dma((3,))]
    sems += [one] * 3 + [pltpu.SemaphoreType.REGULAR, dma((5,)), one]
    return [pltpu.VMEM(d, k) for d, k in shapes] + sems, total


def fused(n_rows_z, scratch, tokens, gain, ids, slot, dropped, gates, wg, wu, wd, sg, su, sd):
    hbm = pl.BlockSpec(memory_space=pl.ANY)
    return pl.pallas_call(
        functools.partial(layer_kernel, n_rows_z),
        out_shape=jax.ShapeDtypeStruct(tokens.shape, tokens.dtype),
        in_specs=[hbm] * 11,
        out_specs=hbm,
        scratch_shapes=scratch,
        compiler_params=pltpu.CompilerParams(
            collective_id=0, has_side_effects=True, vmem_limit_bytes=VMEM_BYTES
        ),
        name="moe_layer",
    )(
        tokens,
        gain[None, :],
        ids.T,
        dropped.T,
        gates.T,
        wg.transpose(0, 2, 1),
        wu.transpose(0, 2, 1),
        wd.transpose(0, 2, 1),
        sg.T,
        su.T,
        sd,
    )


TOP = 6
EXP_DEV = 2
TOK_DEV = 128


norm_eps = 1e-06


def swiglu(left, right):
    return jax.nn.silu(left) * right


def on_device(
    tokens,
    norm_gain,
    expert_ids,
    slot_index,
    dropped,
    gates,
    w_gate,
    w_up,
    w_down,
    shared_gate,
    shared_up,
    shared_down,
):
    n_expert_groups = lax.axis_size("ep")
    experts = EXP_DEV * n_expert_groups
    capacity = TOK_DEV * TOP * 4 // (experts * 3)
    model_width = tokens.shape[1]
    local_rows = tokens.shape[0]
    values = tokens.astype(jnp.float32)
    scale = lax.rsqrt(jnp.mean(values * values, axis=-1, keepdims=True) + norm_eps)
    normed = (values * scale * norm_gain).astype(jnp.bfloat16)
    destination_position = expert_ids * capacity + slot_index
    kept_pair = dropped == 0
    matrix_breadth = lax.iota(jnp.int32, experts * capacity)
    matches = (destination_position[:, :, None] == matrix_breadth[None, None, :]) & kept_pair[
        :, :, None
    ]
    dispatch_table = jnp.any(matches, axis=1).astype(jnp.bfloat16)
    outgoing = lax.dot_general(
        dispatch_table, normed, (((0,), (0,)), ((), ())), preferred_element_type=jnp.float32
    ).astype(jnp.bfloat16)
    boxes = outgoing.reshape(n_expert_groups, EXP_DEV, capacity, model_width)
    received = lax.all_to_all(boxes, "ep", split_axis=0, concat_axis=0, tiled=True)
    gate_all = lax.all_gather(w_gate, "tp", axis=2, tiled=True)
    up_all = lax.all_gather(w_up, "tp", axis=2, tiled=True)
    down_all = lax.all_gather(w_down, "tp", axis=2, tiled=True)
    gate_act = jnp.einsum("iecd,edf->iecf", received, gate_all, preferred_element_type=jnp.float32)
    up_act = jnp.einsum("iecd,edf->iecf", received, up_all, preferred_element_type=jnp.float32)
    hidden = swiglu(gate_act, up_act).astype(jnp.bfloat16)
    expert_out = jnp.einsum(
        "iecf,edf->iecd", hidden, down_all, preferred_element_type=jnp.float32
    ).astype(jnp.bfloat16)
    returned_output = lax.all_to_all(expert_out, "ep", split_axis=0, concat_axis=0, tiled=True)
    returned_rows = returned_output.reshape(experts * capacity, model_width)
    shard_piece = lax.all_gather(normed, "tp", axis=0, tiled=True)
    gate_act = jnp.dot(shard_piece, shared_gate, preferred_element_type=jnp.float32)
    up_act = jnp.dot(shard_piece, shared_up, preferred_element_type=jnp.float32)
    partial_hidden = swiglu(gate_act, up_act).astype(jnp.bfloat16)
    whole_hidden = lax.all_to_all(partial_hidden, "tp", split_axis=0, concat_axis=1, tiled=True)
    shared_out = jnp.dot(whole_hidden, shared_down, preferred_element_type=jnp.float32)
    safe_target = jnp.where(kept_pair, destination_position, 0)
    picked = jnp.take(returned_rows, safe_target.reshape(-1), axis=0).reshape(
        local_rows, TOP, model_width
    )
    kept_weights = jnp.where(kept_pair, gates, jnp.float32(0.0))
    routed = jnp.sum(picked.astype(jnp.float32) * kept_weights[:, :, None], axis=1)
    return (values + shared_out + routed).astype(jnp.bfloat16)


def solution(mesh):
    ep, tp = mesh.shape["ep"], mesh.shape["tp"]
    placed = (
        P(("ep", "tp"), None),
        P(),
        P(("ep", "tp"), None),
        P(("ep", "tp"), None),
        P(("ep", "tp"), None),
        P(("ep", "tp"), None),
        P("ep", None, "tp"),
        P("ep", None, "tp"),
        P("ep", None, "tp"),
        P(None, "tp"),
        P(None, "tp"),
        P(),
    )

    def layer(*args):
        tokens, w_gate, shared_gate = args[0], args[6], args[9]
        n_rows_z = ep // COLS
        scratch, size = scratch_of(
            n_rows_z,
            tokens.shape[0],
            args[2].shape[1],
            tokens.shape[1],
            ep * w_gate.shape[0],
            w_gate.shape[0],
            w_gate.shape[2],
            shared_gate.shape[1],
        )
        spare = 8 * 1024 * 1024
        if tp == 2 * CORES and n_rows_z == 4 and w_gate.shape[0] == 2 and size + spare < VMEM_BYTES:
            return fused(n_rows_z, scratch, *args)
        return on_device(*args)

    return jax.shard_map(
        layer, mesh=mesh, in_specs=placed, out_specs=P(("ep", "tp"), None), check_vma=False
    )
```

```python
import functools

import jax
import jax.numpy as jnp
from jax import lax
from jax.experimental import pallas as pl
from jax.experimental.pallas import tpu as pltpu
from jax.sharding import PartitionSpec as P

MESH = pl.DeviceIdType.MESH
CORES = 2
COLS = 2
VMEM_BYTES = 62 * 1024 * 1024
LANES = 128
SWING = 3

NT = (((1,), (1,)), ((), ()))
NN = (((1,), (0,)), ((), ()))


def dot(a, b, dims):
    return lax.dot_general(a, b, dims, preferred_element_type=jnp.float32)


def flip(index, mask, size):
    out, bit = 0, 1
    while bit < size:
        digit = (index // bit) % 2
        out = out + (1 - digit if mask & bit else digit) * bit
        bit *= 2
    return out


def cuts_of(width):
    inside = width - 6 * LANES
    sizes = [LANES] * 2 + [2 * LANES] * (inside // (2 * LANES)) + [LANES] * 4
    starts = [sum(sizes[:i]) for i in range(len(sizes))]
    return [pl.ds(*cut) for cut in zip(starts, sizes)]


def layer_kernel(
    n_rows_z,
    tokens_in,
    gain_in,
    ids_in,
    dropped_in,
    gates_in,
    w_gate,
    w_up,
    w_down,
    s_gate,
    s_up,
    s_down,
    result,
    tokens,
    gain,
    ids,
    dropped,
    gates,
    out,
    xb,
    wtb,
    gu,
    ga0,
    ga1,
    db,
    hb,
    hl0,
    hl1,
    sb,
    sg,
    su,
    sd,
    sh,
    whid,
    ysend,
    yrecv,
    ypart,
    zsend,
    zrecv,
    zsend2,
    zrecv2,
    own_sem,
    near_send,
    near_recv,
    far_send,
    far_recv,
    pass_send,
    pass_recv,
    z_send,
    z_recv,
    y_send,
    y_recv,
    t_send,
    t_recv,
    h_send,
    h_recv,
    ry_send,
    ry_recv,
    rz_send,
    rz_join,
    rz_recv,
    sw_send,
    sw_join,
    sw_recv,
    go,
    in_sem,
    out_sem,
):
    ep, tp = lax.axis_index("ep"), lax.axis_index("tp")
    z, y = ep // COLS, ep % COLS
    x, core = tp // CORES, tp % CORES
    rows, width = tokens.shape
    experts = w_gate.shape[0]
    hid = w_gate.shape[1]
    shid = s_gate.shape[0]
    cuts = cuts_of(width)
    pieces = len(cuts)
    split = hl0.shape[-1] // 2
    last = experts - 1
    mate = (ep, x * CORES + 1 - core)
    across = (ep, (1 - x) * CORES + core)
    diagonal = (ep, (1 - x) * CORES + 1 - core)
    beside = (z * COLS + 1 - y, tp)
    along = [None] + [(flip(z, r, n_rows_z) * COLS + y, tp) for r in range(1, n_rows_z)]
    at_end = jnp.where(z % 3 == 0, 1, 0)
    inner = at_end == 0
    order = [0, 1, 3 - at_end, 2 + at_end]

    barrier = pltpu.get_barrier_semaphore()
    peers = [mate, across, diagonal, beside] + along[1:]
    for peer in peers:
        pl.semaphore_signal(barrier, inc=1, device_id=peer, device_id_type=MESH)

    def local(src, dst, sem):
        c = pltpu.make_async_copy(src, dst, sem)
        c.start()
        return c

    inputs = [
        local(src, dst, in_sem.at[i])
        for i, (src, dst) in enumerate(
            (
                (tokens_in, tokens),
                (gain_in, gain),
                (ids_in, ids),
                (dropped_in, dropped),
                (gates_in, gates),
            )
        )
    ]
    chunks = []

    def add_chunk(source, e, m, start, size):
        rows_cut = pl.ds(start, size)
        chunks.append((source.at[e, rows_cut], lambda s: gu.at[e, m, s, rows_cut]))

    for e in range(experts):
        add_chunk(w_gate, e, 0, 0, hid)
        if e < last:
            add_chunk(w_up, e, 1, 0, hid)
        else:
            add_chunk(w_up, e, 1, 0, split)
            add_chunk(w_up, e, 1, split, hid - split)
    first_down = len(chunks)
    for cut in cuts:
        chunks.append(
            (w_down.at[:, :, cut], functools.partial(lambda cut, s: db.at[:, s, :, cut], cut))
        )
    n = len(chunks)

    def whole(s):
        return [(w_gate, gu.at[:, 0, s]), (w_up, gu.at[:, 1, s]), (w_down, db.at[:, s])]

    own = [local(src, dst, own_sem.at[i]) for i, (src, dst) in enumerate(whole(0))]
    shared_in = [local(s_gate, sg, own_sem.at[3]), local(s_up, su, own_sem.at[4])]
    who = [tp, mate[1], across[1], diagonal[1]]
    for s in range(4):
        local(
            s_down.at[pl.ds(pl.multiple_of(who[s] * shid, 16), shid), :],
            sd.at[pl.ds(s * shid, shid)],
            own_sem.at[5],
        )

    pl.semaphore_wait(barrier, len(peers))
    def copy_to(src, dst, ssem, rsem, peer):
        return pltpu.make_async_remote_copy(
            src_ref=src,
            dst_ref=dst,
            send_sem=ssem,
            recv_sem=rsem,
            device_id=peer,
            device_id_type=MESH,
        )

    def remote(src, dst, ssem, rsem, peer):
        c = copy_to(src, dst, ssem, rsem, peer)
        c.start()
        return c

    def group(k):
        return 0 if k < first_down else 1

    far = [
        copy_to(source, place(2), far_send.at[group(k)], far_recv.at[k], across)
        for k, (source, place) in enumerate(chunks)
    ]
    late = range(first_down + 3, n)
    for k in [*range(first_down - 1), first_down, first_down - 1, first_down + 1, first_down + 2]:
        far[k].start()

    @pl.when(core == 0)
    def _():
        for k in late:
            far[k].start()

    near = [
        remote(src, dst, near_send.at[i], near_recv.at[i], mate)
        for i, (src, dst) in enumerate(whole(1))
    ]

    for c in inputs:
        c.wait()
    values = tokens[...].astype(jnp.float32)
    scale = lax.rsqrt(jnp.mean(values * values, axis=-1, keepdims=True) + 1e-06)
    xb[0, 0] = (values * scale * gain[...]).astype(jnp.bfloat16)
    table = jnp.zeros(wtb.shape[2:], jnp.float32)
    rows_of = lax.broadcasted_iota(jnp.int32, wtb.shape[2:], 0)
    for k in range(ids.shape[0]):
        hit = (ids[k : k + 1, :] == rows_of) & (dropped[k : k + 1, :] == 0)
        table = table + jnp.where(hit, gates[k : k + 1, :], 0.0)
    wtb[0, 0] = table

    half = rows // 2
    parts = 3

    def part(i, side, slot):
        if i == 0:
            return wtb.at[side, slot]
        return xb.at[side, slot, pl.ds((i - 1) * half, half)]

    routes = [(0, 1, 1), (0, 3, 3), (1, 2, 3), (3, 2, 1), (2, 3, 1)]
    hops = [
        [
            copy_to(
                part(i, 0, src),
                part(i, 0, dst),
                z_send.at[min(k, 1), min(i, 1)],
                z_recv.at[i, dst - 1],
                along[by],
            )
            for i in range(parts)
        ]
        for k, (src, dst, by) in enumerate(routes)
    ]

    def arrived(i, slot):
        copy_to(
            part(i, 0, 0), part(i, 0, slot), z_send.at[0, 0], z_recv.at[i, slot - 1], along[1]
        ).wait_recv()

    def to_side(k, i):
        slot = order[k]
        m = min(i, 1)
        remote(part(i, 0, slot), part(i, 1, slot), y_send.at[m], y_recv.at[m, k], beside)

    def from_side(k):
        for m, ref in enumerate((wtb, xb)):
            slot = ref.at[1, order[k]]
            copy_to(slot, slot, y_send.at[m], y_recv.at[m, k], beside).wait_recv()

    for i in range(parts):
        hops[0][i].start()

    @pl.when(inner)
    def _():
        for i in range(parts):
            hops[1][i].start()

    for i in range(parts):
        to_side(0, i)
    share_near = remote(xb.at[0, 0], sb.at[1], t_send, t_recv.at[0], mate)
    share_far = copy_to(xb.at[0, 0], sb.at[2], t_send, t_recv.at[1], across)

    @pl.when(core == 0)
    def _():
        share_far.start()

    passed = {}

    def pass_on(k):
        far[k].wait_recv()
        place = chunks[k][1]
        passed[k] = remote(place(2), place(3), pass_send.at[group(k)], pass_recv.at[k], mate)

    def column(side, r, e):
        line = jnp.sum(
            jnp.where(rows_of == ep * experts + e, wtb[side, r], 0.0), axis=0, keepdims=True
        )
        return jnp.transpose(jnp.broadcast_to(line, (rows, rows)))[:, 0:1]

    def both_sides(r):
        return jnp.concatenate([xb[0, r], xb[1, r]], axis=0)

    def two_rows(side, q):
        return xb[side, pl.ds(2 * q, 2)].reshape(2 * rows, width)

    def matrix(e, m, pair, start, size):
        picked = gu[e, m, 2 * pair : 2 * pair + 2, start : start + size]
        return picked.reshape(2 * size, width)

    def activate(g, u, r, e):
        weight = jnp.concatenate([column(0, r, e), column(1, r, e)], axis=0)
        return (g * jax.nn.sigmoid(g) * u * weight).astype(jnp.bfloat16)

    def hidden(r, pair, e):
        left = both_sides(r)
        g = dot(left, matrix(e, 0, pair, 0, hid), NT)
        u = dot(left, matrix(e, 1, pair, 0, hid), NT)
        h = activate(g, u, r, e)
        hb[0, e * 2 + pair, r] = h[:rows]
        hb[1, e * 2 + pair, r] = h[rows:]

    def near_hidden(k):
        def body(e, carry):
            hidden(order[k], 0, e)
            return carry

        lax.fori_loop(0, experts, body, 0)

    def far_hidden(first, count):
        def body(i, carry):
            r = i
            for k in range(1, n_rows_z):
                r = jnp.where(i == k, order[k], r)
            hidden(r, 1, 0)
            return carry

        lax.fori_loop(first, first + count, body, 0)

    def last_gate():
        def body(i, carry):
            left = two_rows(i // 2, i % 2)
            ga0[i] = dot(left, matrix(last, 0, 1, 0, split), NT)
            ga1[i] = dot(left, matrix(last, 0, 1, split, hid - split), NT)
            return carry

        lax.fori_loop(0, n_rows_z, body, 0)

    def last_up(stored, start, size, place, side):
        def body(q, carry):
            u = dot(two_rows(side, q), matrix(last, 1, 1, start, size), NT)
            g = stored[2 * side + q]
            weight = [column(side, 2 * q + i, last) for i in range(2)]
            h = g * jax.nn.sigmoid(g) * u * jnp.concatenate(weight, axis=0)
            place[side, pl.ds(2 * q, 2)] = h.astype(jnp.bfloat16).reshape(2, rows, 2 * size)
            return carry

        lax.fori_loop(0, n_rows_z // 2, body, 0)

    def shared_act(left):
        g = dot(left, sg[...], NT)
        u = dot(left, su[...], NT)
        return (g * jax.nn.sigmoid(g) * u).astype(jnp.bfloat16)

    def shared_hidden():
        h = shared_act(jnp.concatenate([xb[0, 0], sb[1]], axis=0))
        sh[0] = h[:rows]
        sh[1] = h[rows:]

    for i in range(2):
        own[i].wait()
        near[i].wait_recv()
    for i in range(parts):
        arrived(i, 1)
        to_side(1, i)

        @pl.when(inner)
        def _(i=i):
            hops[2][i].start()
            arrived(i, 3)
            hops[3][i].start()

    from_side(0)
    near_hidden(0)
    for c in shared_in:
        c.wait()
    share_near.wait_recv()
    shared_hidden()
    share_back = remote(sh.at[1], whid.at[1], h_send, h_recv.at[0], mate)
    pass_on(0)
    for i in range(parts):

        @pl.when(inner)
        def _(i=i):
            arrived(i, 2)
            hops[4][i].start()

        @pl.when(at_end == 1)
        def _(i=i):
            arrived(i, 2)

        to_side(2, i)
    from_side(1)
    near_hidden(1)
    for i in range(parts):

        @pl.when(at_end == 1)
        def _(i=i):
            arrived(i, 3)

        to_side(3, i)
        if i == 1:
            pass_on(1)
            passed[0].wait_recv()
            passed[1].wait_recv()
            far_hidden(0, 2)
    from_side(2)
    near_hidden(2)
    far_hidden(2, 1)
    from_side(3)
    near_hidden(3)
    far_hidden(3, 1)
    pass_on(2)
    passed[2].wait_recv()
    last_gate()
    pass_on(3)
    passed[3].wait_recv()
    for side in range(COLS):
        last_up(ga0, 0, split, hl0, side)
    pass_on(first_down)
    pass_on(first_down - 1)

    @pl.when(core == 0)
    def _():
        pl.semaphore_signal(go, inc=1, device_id=mate, device_id_type=MESH)

    @pl.when(core == 1)
    def _():
        pl.semaphore_wait(go, 1)
        for k in late:
            far[k].start()
        share_far.start()

    passed[first_down - 1].wait_recv()
    last_up(ga1, split, hid - split, hl1, 1)

    def down(c, side):
        cut = cuts[c]
        piece = cut.size

        def body(q, carry):
            total = None

            def add(total, left, e, pair, start, size):
                left = left.reshape(2 * rows, 2 * size)
                right = db[e, 2 * pair : 2 * pair + 2, start : start + size, cut]
                part = dot(left, right.reshape(2 * size, piece), NN)
                return part if total is None else total + part

            two = pl.ds(2 * q, 2)
            for e in range(experts):
                for pair in range(2):
                    if 2 * e + pair < 2 * experts - 1:
                        total = add(total, hb[side, 2 * e + pair, two], e, pair, 0, hid)
            total = add(total, hl0[side, two], last, 1, 0, split)
            total = add(total, hl1[side, two], last, 1, split, hid - split)
            total = total.reshape(2, rows, piece)
            if side:
                ysend[two, :, cut] = total.astype(jnp.bfloat16)
            else:
                ypart[two, :, cut] = total
            return carry

        lax.fori_loop(0, n_rows_z // 2, body, 0)

    end = pieces - 1

    def side_leg(c, r):
        sem = ry_recv.at[c + (n_rows_z - 1 - r if c == end else 0)]
        span = r if c == end else pl.ds(0, n_rows_z)
        return copy_to(
            ysend.at[span, :, cuts[c]], yrecv.at[span, :, cuts[c]], ry_send, sem, beside
        )

    def send_side(c):
        for r in range(n_rows_z - 1, -1, -1) if c == end else (0,):
            side_leg(c, r).start()

    def block(c, r, extra=None):
        cut = cuts[c]
        total = ypart[r, :, cut] + yrecv[r, :, cut].astype(jnp.float32)
        if extra is not None:
            total = total + zrecv[extra, :, cut].astype(jnp.float32)
        zsend[r, :, cut] = total.astype(jnp.bfloat16)

    def leg(c, r, slot, by, sem):
        return copy_to(
            zsend.at[r, :, cuts[c]], zrecv.at[slot, :, cuts[c]], rz_send, sem, along[by]
        )

    def join_sem(c, slot):
        return rz_join.at[c + (1 if c == end and slot == 2 else 0)]

    def last_sem(c):
        return rz_recv.at[max(c - end + 2, 0)]

    def turn(c):
        if c < end:
            side_leg(c, 0).wait_recv()

        @pl.when(at_end == 1)
        def _():
            for r, slot in ((3, 0), (2, 2)):
                if c == end:
                    side_leg(c, r).wait_recv()
                block(c, r)
                leg(c, r, slot, 1, join_sem(c, slot)).start()
            if c == end:
                side_leg(c, 1).wait_recv()
            for k in {end - 1: (), end: (end - 1, end)}.get(c, (c,)):
                block(k, 1)
                leg(k, 1, 1, 1, last_sem(k)).start()

        @pl.when(inner)
        def _():
            if c == end:
                for r in (3, 2, 1):
                    side_leg(c, r).wait_recv()
            block(c, 1)
            leg(c, 1, 1, 1, last_sem(c)).start()

        if c == end:
            side_leg(c, 0).wait_recv()

    def join(c):
        @pl.when(inner)
        def _():
            if c < end:
                both = zrecv.at[pl.ds(0, 2), :, cuts[c]]
                copy_to(both, both, rz_send, join_sem(c, 0), along[1]).wait_recv()
            for r, slot in ((2, 0), (3, 2)):
                if c == end:
                    leg(c, 1, slot, 1, join_sem(c, slot)).wait_recv()
                block(c, r, slot)
                leg(c, r, r, r, last_sem(c)).start()

    def swing_leg(src, slot, by, sem):
        return copy_to(src, zrecv2.at[slot], sw_send, sem, along[by])

    swing = cuts[SWING]

    def swing_out():
        def ahead(r, slot, sem, sem2):
            zsend[r, :, swing] = ypart[r, :, swing].astype(jnp.bfloat16)
            leg(SWING, r, slot, 1, sem).start()
            swing_leg(ysend.at[r, :, swing], slot, 1, sem2).start()

        @pl.when(at_end == 1)
        def _():
            for r, slot in ((3, 0), (2, 2)):
                ahead(r, slot, join_sem(SWING, slot), sw_join)
            ahead(1, 1, last_sem(SWING), sw_recv)

        @pl.when(inner)
        def _():
            ahead(1, 1, last_sem(SWING), sw_recv)

    def swing_join():
        @pl.when(inner)
        def _():
            both = zrecv.at[pl.ds(0, 2), :, swing]
            copy_to(both, both, rz_send, join_sem(SWING, 0), along[1]).wait_recv()
            both = zrecv2.at[pl.ds(0, 2)]
            copy_to(both, both, sw_send, sw_join, along[1]).wait_recv()
            for r, slot in ((2, 0), (3, 2)):
                total = ypart[r, :, swing] + zrecv[slot, :, swing].astype(jnp.float32)
                zsend[r, :, swing] = total.astype(jnp.bfloat16)
                leg(SWING, r, r, r, last_sem(SWING)).start()
                total = ysend[r, :, swing].astype(jnp.float32) + zrecv2[slot].astype(jnp.float32)
                zsend2[r] = total.astype(jnp.bfloat16)
                swing_leg(zsend2.at[r], r, r, sw_recv).start()

    def swing_side():
        return copy_to(zsend2.at[0], yrecv.at[0, :, swing], sw_send, ry_recv.at[SWING], beside)

    def swing_cross():
        both = zrecv2.at[pl.ds(0, 2)]
        copy_to(both, both, sw_send, sw_recv, along[1]).wait_recv()
        total = ysend[0, :, swing].astype(jnp.float32)
        for slot in (1, order[2]):
            total = total + zrecv2[slot].astype(jnp.float32)
        zsend2[0] = total.astype(jnp.bfloat16)
        swing_side().start()

    def base(first, stop, c):
        cut = cuts[c]
        total = ypart[0, :, cut]
        if first == 0:
            total = total + tokens[:, cut].astype(jnp.float32)
        for s in range(first, stop):
            left = sh[0] if s == 0 else whid[s]
            total = total + dot(left, sd[s * shid : (s + 1) * shid, cut], NN)
        ypart[0, :, cut] = total

    def landed(first, stop):
        start = cuts[first].start
        span = pl.ds(start, cuts[stop - 1].start + cuts[stop - 1].size - start)
        both = zrecv.at[pl.ds(0, 2), :, span]
        copy_to(both, both, rz_send, last_sem(first), along[1]).wait_recv()

    def final(c):
        cut = cuts[c]
        total = ypart[0, :, cut] + yrecv[0, :, cut].astype(jnp.float32)
        for slot in (1, order[2]):
            total = total + zrecv[slot, :, cut].astype(jnp.float32)
        out[:, cut] = total.astype(out.dtype)
        local(out.at[:, cut], result.at[:, cut], out_sem)

    steps = {
        2: [lambda: turn(0)],
        3: [swing_out, lambda: turn(1)],
        4: [lambda: turn(2), lambda: join(0)],
        6: [lambda: turn(4)],
        7: [swing_join],
        8: [lambda: join(1), lambda: turn(5)],
        end: [lambda: join(2), lambda: turn(6), swing_cross],
    }
    rest = [lambda: turn(7), lambda: join(4), lambda: turn(8), lambda: join(5)]
    steps[end] += rest
    own[2].wait()
    near[2].wait_recv()
    for c in range(pieces):
        k = first_down + c
        if k not in passed:
            pass_on(k)
        passed[k].wait_recv()
        down(c, 1)
        if c != SWING:
            send_side(c)
        if c == 0:
            pass_on(k + 1)
            last_up(ga1, split, hid - split, hl1, 0)
        down(c, 0)
        if c == 0:
            pltpu.make_async_copy(s_down, sd, own_sem.at[5]).wait()
            share_back.wait_recv()
        base(0, 2, c)
        if 0 < c < end:
            pass_on(k + 1)
        for step in steps.get(c, []):
            step()

    turn(end - 1)
    share_far.wait_recv()
    share_on = remote(sb.at[2], sb.at[3], t_send, t_recv.at[2], mate)
    join(6)
    sh[2] = shared_act(sb[2])
    remote(sh.at[2], whid.at[2], h_send, h_recv.at[1], across)
    share_on.wait_recv()
    sh[3] = shared_act(sb[3])
    remote(sh.at[3], whid.at[3], h_send, h_recv.at[1], diagonal)
    join(7)
    turn(end)
    for c in range(end - 2, end + 1):
        join(c)
    swing_side().wait_recv()
    both_back = whid.at[pl.ds(2, 2)]
    copy_to(both_back, both_back, h_send, h_recv.at[1], across).wait_recv()
    for c in range(pieces):
        base(2, 4, c)
    landed(0, end - 1)
    for c in range(end - 1):
        final(c)
    for c in (end - 1, end):
        landed(c, c + 1)
        final(c)

    def drain(ref, sem):
        copy_to(ref, ref, sem, near_recv.at[0], mate).wait_send()

    for c in near:
        c.wait_send()
    for sems in (far_send, pass_send):
        drain(gu.at[:, :, 2], sems.at[0])
        drain(db.at[:, 2], sems.at[1])
    for m, ref in enumerate((wtb, xb)):
        drain(ref.at[0, 0], z_send.at[0, m])
        drain(ref.at[0], y_send.at[m])
    drain(sb.at[pl.ds(0, 3)], t_send)
    drain(sh.at[pl.ds(0, 3)], h_send)
    drain(ysend.at[:, :, pl.ds(0, width - swing.size)], ry_send)
    drain(zsend2, sw_send)
    drain(zsend.at[pl.ds(1, 3)], rz_send)

    @pl.when(inner)
    def _():
        for m, ref in enumerate((wtb, xb)):
            drain(ref.at[0], z_send.at[1, m])

    pltpu.make_async_copy(out, result, out_sem).wait()


def scratch_of(n_rows_z, rows, top, width, n_experts, experts, hid, shid):
    bf, f4 = jnp.bfloat16, jnp.float32
    pieces = len(cuts_of(width))
    lines = n_experts
    split = hid - hid // 32 * 16
    pad = lambda v: -(-v // 128) * 128
    shapes = [
        ((rows, width), bf),
        ((1, width), f4),
        ((top, rows), jnp.int32),
        ((top, rows), jnp.int32),
        ((top, rows), f4),
        ((rows, width), bf),
        ((COLS, n_rows_z, rows, width), bf),
        ((COLS, n_rows_z, lines, rows), f4),
        ((experts, 2, 4, hid, width), bf),
        ((n_rows_z, 2 * rows, 2 * split), f4),
        ((n_rows_z, 2 * rows, 2 * (hid - split)), f4),
        ((experts, 4, hid, width), bf),
        ((COLS, 2 * experts - 1, n_rows_z, rows, 2 * hid), bf),
        ((COLS, n_rows_z, rows, 2 * split), bf),
        ((COLS, n_rows_z, rows, 2 * (hid - split)), bf),
        ((4, rows, width), bf),
        ((shid, width), bf),
        ((shid, width), bf),
        ((4 * shid, width), bf),
        ((4, rows, shid), bf),
        ((4, rows, shid), bf),
        ((n_rows_z, rows, width), bf),
        ((n_rows_z, rows, width), bf),
        ((n_rows_z, rows, width), f4),
        ((n_rows_z, rows, width), bf),
        ((n_rows_z, rows, width), bf),
        ((n_rows_z, rows, 2 * LANES), bf),
        ((n_rows_z, rows, 2 * LANES), bf),
    ]
    total = 0
    for dims, kind in shapes:
        size = pad(dims[-1]) * jnp.dtype(kind).itemsize
        for d in dims[:-1]:
            size *= d
        total += size
    n = 2 * experts + 1 + pieces
    dma = pltpu.SemaphoreType.DMA
    one = pltpu.SemaphoreType.DMA
    sems = [dma((6,)), dma((3,)), dma((3,)), dma((2,)), dma((n,)), dma((2,)), dma((n,))]
    sems += [dma((2, 2)), dma((3, n_rows_z - 1)), dma((2,)), dma((2, n_rows_z))]
    sems += [one, dma((3,)), one, dma((2,))]
    sems += [one, dma((pieces + n_rows_z - 1,)), one, dma((pieces + 1,)), dma((3,))]
    sems += [one] * 3 + [pltpu.SemaphoreType.REGULAR, dma((5,)), one]
    return [pltpu.VMEM(d, k) for d, k in shapes] + sems, total


def fused(n_rows_z, scratch, tokens, gain, ids, slot, dropped, gates, wg, wu, wd, sg, su, sd):
    hbm = pl.BlockSpec(memory_space=pl.ANY)
    return pl.pallas_call(
        functools.partial(layer_kernel, n_rows_z),
        out_shape=jax.ShapeDtypeStruct(tokens.shape, tokens.dtype),
        in_specs=[hbm] * 11,
        out_specs=hbm,
        scratch_shapes=scratch,
        compiler_params=pltpu.CompilerParams(
            collective_id=0, has_side_effects=True, vmem_limit_bytes=VMEM_BYTES
        ),
        name="moe_layer",
    )(
        tokens,
        gain[None, :],
        ids.T,
        dropped.T,
        gates.T,
        wg.transpose(0, 2, 1),
        wu.transpose(0, 2, 1),
        wd.transpose(0, 2, 1),
        sg.T,
        su.T,
        sd,
    )


TOP = 6
EXP_DEV = 2
TOK_DEV = 128


norm_eps = 1e-06


def swiglu(left, right):
    return jax.nn.silu(left) * right


def on_device(
    tokens,
    norm_gain,
    expert_ids,
    slot_index,
    dropped,
    gates,
    w_gate,
    w_up,
    w_down,
    shared_gate,
    shared_up,
    shared_down,
):
    n_expert_groups = lax.axis_size("ep")
    experts = EXP_DEV * n_expert_groups
    capacity = TOK_DEV * TOP * 4 // (experts * 3)
    model_width = tokens.shape[1]
    local_rows = tokens.shape[0]
    values = tokens.astype(jnp.float32)
    scale = lax.rsqrt(jnp.mean(values * values, axis=-1, keepdims=True) + norm_eps)
    normed = (values * scale * norm_gain).astype(jnp.bfloat16)
    destination_position = expert_ids * capacity + slot_index
    kept_pair = dropped == 0
    matrix_breadth = lax.iota(jnp.int32, experts * capacity)
    matches = (destination_position[:, :, None] == matrix_breadth[None, None, :]) & kept_pair[
        :, :, None
    ]
    dispatch_table = jnp.any(matches, axis=1).astype(jnp.bfloat16)
    outgoing = lax.dot_general(
        dispatch_table, normed, (((0,), (0,)), ((), ())), preferred_element_type=jnp.float32
    ).astype(jnp.bfloat16)
    boxes = outgoing.reshape(n_expert_groups, EXP_DEV, capacity, model_width)
    received = lax.all_to_all(boxes, "ep", split_axis=0, concat_axis=0, tiled=True)
    gate_all = lax.all_gather(w_gate, "tp", axis=2, tiled=True)
    up_all = lax.all_gather(w_up, "tp", axis=2, tiled=True)
    down_all = lax.all_gather(w_down, "tp", axis=2, tiled=True)
    gate_act = jnp.einsum("iecd,edf->iecf", received, gate_all, preferred_element_type=jnp.float32)
    up_act = jnp.einsum("iecd,edf->iecf", received, up_all, preferred_element_type=jnp.float32)
    hidden = swiglu(gate_act, up_act).astype(jnp.bfloat16)
    expert_out = jnp.einsum(
        "iecf,edf->iecd", hidden, down_all, preferred_element_type=jnp.float32
    ).astype(jnp.bfloat16)
    returned_output = lax.all_to_all(expert_out, "ep", split_axis=0, concat_axis=0, tiled=True)
    returned_rows = returned_output.reshape(experts * capacity, model_width)
    shard_piece = lax.all_gather(normed, "tp", axis=0, tiled=True)
    gate_act = jnp.dot(shard_piece, shared_gate, preferred_element_type=jnp.float32)
    up_act = jnp.dot(shard_piece, shared_up, preferred_element_type=jnp.float32)
    partial_hidden = swiglu(gate_act, up_act).astype(jnp.bfloat16)
    whole_hidden = lax.all_to_all(partial_hidden, "tp", split_axis=0, concat_axis=1, tiled=True)
    shared_out = jnp.dot(whole_hidden, shared_down, preferred_element_type=jnp.float32)
    safe_target = jnp.where(kept_pair, destination_position, 0)
    picked = jnp.take(returned_rows, safe_target.reshape(-1), axis=0).reshape(
        local_rows, TOP, model_width
    )
    kept_weights = jnp.where(kept_pair, gates, jnp.float32(0.0))
    routed = jnp.sum(picked.astype(jnp.float32) * kept_weights[:, :, None], axis=1)
    return (values + shared_out + routed).astype(jnp.bfloat16)


def solution(mesh):
    ep, tp = mesh.shape["ep"], mesh.shape["tp"]
    placed = (
        P(("ep", "tp"), None),
        P(),
        P(("ep", "tp"), None),
        P(("ep", "tp"), None),
        P(("ep", "tp"), None),
        P(("ep", "tp"), None),
        P("ep", None, "tp"),
        P("ep", None, "tp"),
        P("ep", None, "tp"),
        P(None, "tp"),
        P(None, "tp"),
        P(),
    )

    def layer(*args):
        tokens, w_gate, shared_gate = args[0], args[6], args[9]
        n_rows_z = ep // COLS
        scratch, size = scratch_of(
            n_rows_z,
            tokens.shape[0],
            args[2].shape[1],
            tokens.shape[1],
            ep * w_gate.shape[0],
            w_gate.shape[0],
            w_gate.shape[2],
            shared_gate.shape[1],
        )
        spare = 8 * 1024 * 1024
        if tp == 2 * CORES and n_rows_z == 4 and w_gate.shape[0] == 2 and size + spare < VMEM_BYTES:
            return fused(n_rows_z, scratch, *args)
        return on_device(*args)

    return jax.shard_map(
        layer, mesh=mesh, in_specs=placed, out_specs=P(("ep", "tp"), None), check_vma=False
    )
```
